256 devices in a mesh: trial: 4 (over y), rows: 16 (over z, core), cols: 4 (over x).
Axes of the slice: x: 4, y: 4, z: 8, core: 2. Of those that a mesh axis runs over, the one named last changes fastest.
Arguments:
- weight_gate: float32 [8192, 8192], P(('trial', 'rows'), 'cols'), parts along dimension 0, may hold values from -0.1875 to 0.1875
- moment_gate: float32 [8192, 8192], P(('trial', 'rows'), 'cols'), parts along dimension 0, may hold values from -6 to 6
- square_gate: float32 [8192, 8192], P(('trial', 'rows'), 'cols'), parts along dimension 0, may hold values from 0.1 to 10
- weight_up: float32 [8192, 8192], P(('trial', 'rows'), 'cols'), parts along dimension 0, may hold values from -0.1875 to 0.1875
- moment_up: float32 [8192, 8192], P(('trial', 'rows'), 'cols'), parts along dimension 0, may hold values from -6 to 6
- square_up: float32 [8192, 8192], P(('trial', 'rows'), 'cols'), parts along dimension 0, may hold values from 0.1 to 10
- norm_gain: float32 [8192], P(('trial', 'rows')), parts along dimension 0, may hold values from 0.25 to 1.75
Outputs:
- serving_gate: bfloat16 [8192, 8192], P('trial', 'cols'), parts along dimension 0
- serving_up: bfloat16 [8192, 8192], P('trial', 'cols'), parts along dimension 0
- column_gate: float32 [32768], P(('trial', 'cols')), parts along dimension 0
- column_up: float32 [32768], P(('trial', 'cols')), parts along dimension 0
The draws below stay inside these ranges and needn't reach their ends.
There are 4 independent parts, one for each index of `trial`. The reference program is written for one: setup_inputs(seed, part) draws one part's arguments, and reference() takes and returns one part's arrays. A program takes and returns all parts, laid end to end along the dimension named above; each array names one. Nothing has to cross between parts.
All inputs are finite; a program needn't handle non-finite values. Where the reference program divides by a largest or mean magnitude, that divisor is 1e-20 or more.
Results may differ from the reference program's by a relative error of at most 0.001.
Values may be sent and summed in bfloat16 or wider, within the bound.
A program may use at most 128 MiB of HBM per device.

```python
import math
import jax
import jax.numpy as jnp
from jax import lax

D_MODEL = 2048
D_INNER = 8192


def strengthened(array, stream_key, source, target, blocks, factor):
    def block_of(dim):
        return (jnp.arange(array.shape[dim]) // (array.shape[dim] // blocks)).reshape((-1,) + (1,) * (array.ndim - 1 - dim))

    first = jax.random.permutation(stream_key, blocks)[block_of(target)]
    far = (block_of(target) + blocks // 2) % blocks
    return jnp.where((block_of(source) == first) | (block_of(source) == far), factor * array, array)


def shard_levels(stream_key, extent, cuts, least, high):
    def one(axis_at, shards_of):
        draws = jax.random.uniform(jax.random.fold_in(jax.random.fold_in(stream_key, 6), axis_at), (shards_of,), jnp.float32, least / len(cuts), high / len(cuts))
        return jnp.repeat(jnp.exp(draws), extent[axis_at] // shards_of).reshape((-1,) + (1,) * (len(extent) - axis_at - 1))

    level = one(*cuts[0])
    for cut in cuts[1:]:
        level = level * one(*cut)
    return level


def gaussian(own_key, extent, width, bound, split=(), held_as=jnp.bfloat16):
    drawn = jax.random.normal(own_key, extent, jnp.float32) * width
    if len(split) > 0:
        drawn = shard_levels(own_key, extent, split, -0.22, 0.18) * drawn
    return jnp.clip(drawn, min=-bound, max=bound).astype(held_as)


def bell_draw_with(key, extent, width, bound, shards, heavy, kind=jnp.bfloat16):
    values = width * jax.random.normal(key, extent, jnp.float32)
    if shards:
        values = values * shard_levels(key, extent, shards, -0.22, 0.18)
    return jnp.clip(strengthened(values, jax.random.fold_in(key, 3), *heavy), -bound, bound).astype(kind)


def setup_inputs(seed: int = 0, part: int = 0) -> dict:
    splits = jax.random.split(jax.random.key(seed), 8)
    own_keys = jax.random.split(jax.random.fold_in(splits[7], part), 8)
    return {
        "weight_gate": bell_draw_with(own_keys[0], (D_MODEL, D_INNER), D_MODEL ** -0.5, 0.1875, ((0, 16), (1, 4)), (0, 1, 16, 2.0), jnp.float32),
        "moment_gate": gaussian(own_keys[1], (D_MODEL, D_INNER), 1.0, 6.0, ((0, 16), (1, 4)), jnp.float32),
        "square_gate": jnp.clip(jnp.exp(math.log(10.0) - 4.6051702 * jax.random.uniform(own_keys[2], (D_MODEL, D_INNER), jnp.float32) ** shard_levels(own_keys[2], (D_MODEL, D_INNER), ((0, 16), (1, 4)), -0.2, 0.2)), 0.1, 10.0),
        "weight_up": bell_draw_with(own_keys[3], (D_MODEL, D_INNER), D_MODEL ** -0.5, 0.1875, ((0, 16), (1, 4)), (0, 1, 16, 2.0), jnp.float32),
        "moment_up": gaussian(own_keys[4], (D_MODEL, D_INNER), 1.0, 6.0, ((0, 16), (1, 4)), jnp.float32),
        "square_up": jnp.clip(jnp.exp(math.log(10.0) - 4.6051702 * jax.random.uniform(own_keys[5], (D_MODEL, D_INNER), jnp.float32) ** shard_levels(own_keys[5], (D_MODEL, D_INNER), ((0, 16), (1, 4)), -0.2, 0.2)), 0.1, 10.0),
        "norm_gain": jnp.clip(1.0 + 0.15 * jax.random.normal(own_keys[6], (D_MODEL,), jnp.float32), 0.25, 1.75),
    }


learn_rate = 0.02
decay_rate = 0.05
tiny_value = 1e-08

def reference(weight_gate, moment_gate, square_gate, weight_up, moment_up, square_up, norm_gain):
    whole_gate = weight_gate - learn_rate * (moment_gate / (jnp.sqrt(square_gate) + tiny_value) + decay_rate * weight_gate)
    whole_up = weight_up - learn_rate * (moment_up / (jnp.sqrt(square_up) + tiny_value) + decay_rate * weight_up)
    whole_gained_gate = whole_gate * norm_gain[:, None]
    whole_gained_up = whole_up * norm_gain[:, None]
    column_gate = lax.optimization_barrier(jnp.sum(jnp.abs(whole_gained_gate), axis=0)) / D_MODEL
    serving_gate = (whole_gained_gate / column_gate).astype(jnp.bfloat16)
    column_up = lax.optimization_barrier(jnp.sum(jnp.abs(whole_gained_up), axis=0)) / D_MODEL
    serving_up = (whole_gained_up / column_up).astype(jnp.bfloat16)
    return (serving_gate, serving_up, column_gate, column_up)
```

```python
import functools

import jax
import jax.numpy as jnp
from jax import lax
from jax.experimental import pallas as pl
from jax.experimental.pallas import tpu as pltpu
from jax.sharding import PartitionSpec as P

D_MODEL = 2048
learn_rate = 0.02
decay_rate = 0.05
tiny_value = 1e-08

MESH = pl.DeviceIdType.MESH
F32, BF16 = jnp.float32, jnp.bfloat16

CHIPS = 8
PIECES = 4
CHUNK = 512


def gather_kernel(
    wg, mg, sg, wu, mu, su, gain_hbm,
    out_g, out_u, scale_g, scale_u,
    held, plain, gain, gain_t, part, pair_in, slots,
    load_sem, gain_sem, pair_s, pair_r, slot_s, slot_r, scale_s, scale_r,
    right_s, right_r, left_s, left_r, side_s, side_r,
):
    rows, width = wg.shape
    half = width // 2
    me = lax.axis_index("rows")
    chip, core = me // 2, me % 2
    partner = chip * 2 + (1 - core)
    outs, scales = (out_g, out_u), (scale_g, scale_u)
    sources = ((wg, mg, sg), (wu, mu, su))

    def at(c):
        return lax.rem(c + CHIPS, CHIPS)

    def peer(distance):
        return at(chip + distance) * 2 + core

    gain_copy = pltpu.make_async_copy(gain_hbm, gain, gain_sem)
    gain_copy.start()
    loads = []
    for q in range(2):
        for k in range(width // CHUNK):
            cols = pl.ds(k * CHUNK, CHUNK)
            trio = [
                pltpu.make_async_copy(
                    sources[q][i].at[:, cols], held.at[q, i, :, cols], load_sem.at[q, k, i]
                )
                for i in range(3)
            ]
            for copy in trio:
                copy.start()
            loads.append(trio)

    barrier = pltpu.get_barrier_semaphore()
    pl.semaphore_signal(barrier, inc=1, device_id={"rows": partner}, device_id_type=MESH)
    for d in range(1, CHIPS):
        pl.semaphore_signal(barrier, inc=1, device_id={"rows": peer(d)}, device_id_type=MESH)

    gain_copy.wait()
    gain_t[...] = jnp.broadcast_to(gain[...], (rows, rows)).T

    def update(q, k):
        for copy in loads[q * (width // CHUNK) + k]:
            copy.wait()

        @pl.loop(k * CHUNK // 128, (k + 1) * CHUNK // 128)
        def _(j):
            cols = pl.ds(pl.multiple_of(j * 128, 128), 128)
            w = held[q, 0, :, cols]
            m = held[q, 1, :, cols]
            s = held[q, 2, :, cols]
            whole = w - learn_rate * (m / (jnp.sqrt(s) + tiny_value) + decay_rate * w)
            gained = whole * gain_t[...]
            plain[q, :, cols] = gained
            part[q, :, cols] = jnp.sum(jnp.abs(gained), axis=0, keepdims=True)

    def cols_of(h):
        which = (core + h) % 2
        return pl.ds(pl.multiple_of(which * half, half), half)

    mine, other = cols_of(0), cols_of(1)

    def pair_copy(q):
        return pltpu.make_async_remote_copy(
            src_ref=part.at[q, :, other], dst_ref=pair_in.at[q],
            send_sem=pair_s.at[q], recv_sem=pair_r.at[q],
            device_id={"rows": partner}, device_id_type=MESH,
        )

    def slot_copy(q, d):
        return pltpu.make_async_remote_copy(
            src_ref=slots.at[q, 0], dst_ref=slots.at[q, d],
            send_sem=slot_s.at[q, d - 1], recv_sem=slot_r.at[q, d - 1],
            device_id={"rows": peer(d)}, device_id_type=MESH,
        )

    def scale_copy(q, where):
        return pltpu.make_async_remote_copy(
            src_ref=scales[q].at[:, where], dst_ref=scales[q].at[:, where],
            send_sem=scale_s.at[q], recv_sem=scale_r.at[q],
            device_id={"rows": partner}, device_id_type=MESH,
        )

    def block(q, origin_chip, origin_core, h):
        start = pl.multiple_of((origin_chip * 2 + origin_core) * rows, rows)
        return outs[q].at[pl.ds(start, rows), cols_of(h)]

    def ring_copy(step, p, sign):
        q, h = p // 2, p % 2
        ref = block(q, at(chip - sign * step), core, h)
        s, r = (right_s, right_r) if sign > 0 else (left_s, left_r)
        return pltpu.make_async_remote_copy(
            src_ref=ref, dst_ref=ref,
            send_sem=s.at[step, p], recv_sem=r.at[step, p],
            device_id={"rows": peer(sign)}, device_id_type=MESH,
        )

    def ring_arrival(step, p, sign):
        q, h = p // 2, p % 2
        ref = block(q, at(chip - sign * (step + 1)), core, h)
        s, r = (right_s, right_r) if sign > 0 else (left_s, left_r)
        return pltpu.make_async_remote_copy(
            src_ref=ref, dst_ref=ref,
            send_sem=s.at[step, p], recv_sem=r.at[step, p],
            device_id={"rows": peer(sign)}, device_id_type=MESH,
        )

    def side_copy(offset, p, arriving=False):
        q, h = p // 2, p % 2
        if arriving:
            ref = block(q, at(chip + offset), 1 - core, 1 - h)
            ref = outs[q].at[
                pl.ds(pl.multiple_of((at(chip + offset) * 2 + 1 - core) * rows, rows), rows),
                cols_of(1 - h),
            ]
        else:
            ref = block(q, at(chip + offset), core, h)
        index = offset % CHIPS
        return pltpu.make_async_remote_copy(
            src_ref=ref, dst_ref=ref,
            send_sem=side_s.at[index, p], recv_sem=side_r.at[index, p],
            device_id={"rows": partner}, device_id_type=MESH,
        )

    def pair_sum(q):
        pair_copy(q).wait_recv()
        slots[q, 0] = part[q, :, mine] + pair_in[q]
        for d in (4, 3, 5, 2, 6, 1, 7):
            slot_copy(q, d).start()

    def total(q):
        for d in range(1, CHIPS):
            slot_copy(q, d).wait_recv()
        acc = jnp.zeros((1, half), F32)
        for c in range(CHIPS):
            acc = acc + slots[q, at(chip - c)]
        scales[q][:, mine] = acc / D_MODEL
        scale_copy(q, mine).start()

    def narrow(p):
        q, h = p // 2, p % 2
        which = (core + h) % 2
        start = pl.multiple_of(me * rows, rows)

        @pl.loop(0, half // 128)
        def _(j):
            cols = pl.ds(pl.multiple_of(which * half + j * 128, 128), 128)
            inverse = 1.0 / scales[q][:, cols]
            outs[q][pl.ds(start, rows), cols] = (plain[q, :, cols] * inverse).astype(BF16)

    def send_own(p):
        narrow(p)
        ring_copy(0, p, 1).start()
        ring_copy(0, p, -1).start()
        side_copy(0, p).start()

    for k in range(width // CHUNK):
        update(0, k)
    pl.semaphore_wait(barrier, CHIPS)
    pair_copy(0).start()
    update(1, 0)
    pair_sum(0)
    for k in range(1, width // CHUNK):
        update(1, k)
    pair_copy(1).start()
    pair_sum(1)
    total(0)
    send_own(0)
    scale_copy(0, other).wait_recv()
    send_own(1)
    total(1)
    send_own(2)
    scale_copy(1, other).wait_recv()
    send_own(3)

    sent = [(0, p, sign) for p in range(PIECES) for sign in (1, -1)]
    handed = [(0, p) for p in range(PIECES)]
    for step in range(CHIPS // 2):
        for p in range(PIECES):
            for sign in (1, -1):
                last = step == CHIPS // 2 - 1
                if last and (p < PIECES // 2) != (sign > 0):
                    continue
                ring_arrival(step, p, sign).wait_recv()
                on = step + 1
                if on < CHIPS // 2 - 1 or (on == CHIPS // 2 - 1 and (p < PIECES // 2) == (sign > 0)):
                    ring_copy(on, p, sign).start()
                    sent.append((on, p, sign))
                offset = -sign * (step + 1)
                side_copy(offset, p).start()
                handed.append((offset, p))
    for offset, p in handed:
        side_copy(offset, p, arriving=True).wait_recv()
    for step, p, sign in sent:
        ring_copy(step, p, sign).wait_send()
    for offset, p in handed:
        side_copy(offset, p).wait_send()
    for q in range(2):
        pair_copy(q).wait_send()
        scale_copy(q, mine).wait_send()
        for d in range(1, CHIPS):
            slot_copy(q, d).wait_send()


def write_kernel(g, u, a, b, g_out, u_out, a_out, b_out, sems):
    parts = 4
    rows = g.shape[0] // parts
    copies = [
        pltpu.make_async_copy(a, a_out, sems.at[2 * parts]),
        pltpu.make_async_copy(b, b_out, sems.at[2 * parts + 1]),
    ]
    for i, (src, dst) in enumerate(((g, g_out), (u, u_out))):
        for k in range(parts):
            where = pl.ds(k * rows, rows)
            copies.append(pltpu.make_async_copy(src.at[where], dst.at[where], sems.at[i * parts + k]))
    for copy in copies:
        copy.start()
    for copy in copies:
        copy.wait()


def shards(weight_gate, moment_gate, square_gate, weight_up, moment_up, square_up, norm_gain):
    rows, width = weight_gate.shape
    total_rows = rows * lax.axis_size("rows")
    half = width // 2
    any_spec = pl.BlockSpec(memory_space=pl.ANY)
    hbm_spec = pl.BlockSpec(memory_space=pltpu.HBM)
    vmem_spec = pl.BlockSpec(memory_space=pltpu.VMEM)
    dma = pltpu.SemaphoreType.DMA
    g, u, a, b = pl.pallas_call(
        gather_kernel,
        name="gather",
        out_shape=(
            pltpu.VMEM((total_rows, width), BF16),
            pltpu.VMEM((total_rows, width), BF16),
            pltpu.VMEM((1, width), F32),
            pltpu.VMEM((1, width), F32),
        ),
        in_specs=[hbm_spec] * 7,
        out_specs=(vmem_spec,) * 4,
        scratch_shapes=[
            pltpu.VMEM((2, 3, rows, width), F32),
            pltpu.VMEM((2, rows, width), F32),
            pltpu.VMEM((1, rows), F32),
            pltpu.VMEM((rows, rows), F32),
            pltpu.VMEM((2, 1, width), F32),
            pltpu.VMEM((2, 1, half), F32),
            pltpu.VMEM((2, CHIPS, 1, half), F32),
            dma((2, width // CHUNK, 3)), dma,
            dma((2,)), dma((2,)),
            dma((2, CHIPS - 1)), dma((2, CHIPS - 1)),
            dma((2,)), dma((2,)),
            dma((CHIPS // 2, PIECES)), dma((CHIPS // 2, PIECES)),
            dma((CHIPS // 2, PIECES)), dma((CHIPS // 2, PIECES)),
            dma((CHIPS, PIECES)), dma((CHIPS, PIECES)),
        ],
        compiler_params=pltpu.CompilerParams(
            collective_id=0, has_side_effects=True, vmem_limit_bytes=14 * 2**20
        ),
    )(weight_gate, moment_gate, square_gate, weight_up, moment_up, square_up, norm_gain.reshape(1, rows))
    g, u, a, b = pl.pallas_call(
        write_kernel,
        name="write",
        out_shape=(
            jax.ShapeDtypeStruct((total_rows, width), BF16),
            jax.ShapeDtypeStruct((total_rows, width), BF16),
            jax.ShapeDtypeStruct((1, width), F32),
            jax.ShapeDtypeStruct((1, width), F32),
        ),
        in_specs=[vmem_spec] * 4,
        out_specs=(any_spec,) * 4,
        scratch_shapes=[dma((10,))],
        compiler_params=pltpu.CompilerParams(vmem_limit_bytes=2 * 2**20),
    )(g, u, a, b)
    return g, u, a.reshape(width), b.reshape(width)


def solution(mesh):
    return jax.shard_map(
        shards,
        mesh=mesh,
        in_specs=(
            P(("trial", "rows"), "cols"),
            P(("trial", "rows"), "cols"),
            P(("trial", "rows"), "cols"),
            P(("trial", "rows"), "cols"),
            P(("trial", "rows"), "cols"),
            P(("trial", "rows"), "cols"),
            P(("trial", "rows")),
        ),
        out_specs=(
            P("trial", "cols"),
            P("trial", "cols"),
            P(("trial", "cols")),
            P(("trial", "cols")),
        ),
        check_vma=False,
    )
```

```python
import functools

import jax
import jax.numpy as jnp
from jax import lax
from jax.experimental import pallas as pl
from jax.experimental.pallas import tpu as pltpu
from jax.sharding import PartitionSpec as P

D_MODEL = 2048
learn_rate = 0.02
decay_rate = 0.05
tiny_value = 1e-08

MESH = pl.DeviceIdType.MESH
F32, BF16 = jnp.float32, jnp.bfloat16

CHIPS = 8
GROUPS = 4
PIECES = 8
CHUNK = 512
AHEAD = 3
RAW = 48
SLICE = 16


def gather_kernel(
    wg, mg, sg, wu, mu, su, gain_hbm,
    out_g, out_u, scale_g, scale_u,
    held, plain, gain, gain_t, part, slots, pair_in, pair_slots, raw_in,
    load_sem, gain_sem, pair_s, pair_r, slot_s, slot_r, scale_s, scale_r,
    raw_s, raw_r, rest_s, rest_r, ring_s, ring_r, last_r, side_s, side_r,
):
    rows, width = wg.shape
    wide = width * 2 // GROUPS
    half = wide // 2
    chunks = width // CHUNK
    me = lax.axis_index("rows")
    chip, core = me // 2, me % 2
    partner = chip * 2 + (1 - core)
    outs, scales = (out_g, out_u), (scale_g, scale_u)
    sources = ((wg, mg, sg), (wu, mu, su))

    def at(c):
        return lax.rem(c + CHIPS, CHIPS)

    def device(r):
        return dict(device_id={"rows": r}, device_id_type=MESH)

    def take(ref, sem):
        pltpu.make_async_copy(ref, ref, sem).wait()

    def load(n):
        q, k = n // chunks, n % chunks
        cols = pl.ds(k * CHUNK, CHUNK)
        for i in range(3):
            pltpu.make_async_copy(
                sources[q][i].at[:, cols], held.at[q, i, :, cols], load_sem.at[n % (AHEAD + 1)]
            ).start()

    gain_copy = pltpu.make_async_copy(gain_hbm, gain, gain_sem)
    gain_copy.start()
    for n in range(AHEAD):
        load(n)

    barrier = pltpu.get_barrier_semaphore()
    for d in (4, 3, 5, 2, 6, 1, 7):
        for h in range(2):
            pl.semaphore_signal(barrier, inc=1, **device(at(chip + d) * 2 + h))
    pl.semaphore_signal(barrier, inc=1, **device(partner))

    gain_copy.wait()
    gain_t[...] = jnp.broadcast_to(gain[...], (rows, rows)).T

    def update(n):
        q, k = n // chunks, n % chunks
        if n + AHEAD < 2 * chunks:
            load(n + AHEAD)
        block = held.at[q, :, :, pl.ds(k * CHUNK, CHUNK)]
        pltpu.make_async_copy(block, block, load_sem.at[n % (AHEAD + 1)]).wait()

        @pl.loop(k * CHUNK // 128, (k + 1) * CHUNK // 128)
        def _(j):
            cols = pl.ds(pl.multiple_of(j * 128, 128), 128)
            w = held[q, 0, :, cols]
            m = held[q, 1, :, cols]
            s = held[q, 2, :, cols]
            whole = w - learn_rate * (m / (jnp.sqrt(s) + tiny_value) + decay_rate * w)
            gained = whole * gain_t[...]
            plain[q, :, cols] = gained
            part[q, :, cols] = jnp.sum(jnp.abs(gained), axis=0, keepdims=True)

    def start_of(g, h):
        return (g % (GROUPS // 2)) * wide + (core + h) % 2 * half

    def cols_of(g, h):
        return pl.ds(pl.multiple_of(start_of(g, h), half), half)

    far_first = (4, 3, 5, 2, 6, 1, 7)

    def part_of(g, where):
        return part.at[g // (GROUPS // 2), :, where]

    def first_copy(where, target):
        return pltpu.make_async_remote_copy(
            src_ref=part_of(0, where), dst_ref=slots.at[me],
            send_sem=slot_s, recv_sem=slot_r.at[0], **device(target),
        )

    def send_first():
        for d in far_first:
            for h in range(2):
                first_copy(pl.ds(h * half, half), at(chip + d) * 2 + h).start()
        first_copy(cols_of(0, 1), partner).start()
        slots[me] = part[0, :, cols_of(0, 0)]

    def pair_copy(g):
        return pltpu.make_async_remote_copy(
            src_ref=part_of(g, cols_of(g, 1)), dst_ref=pair_in.at[g - 1],
            send_sem=pair_s, recv_sem=pair_r.at[g - 1], **device(partner),
        )

    def send_pair(g):
        pair_copy(g).wait_recv()
        pair_slots[g - 1, chip] = part[g // (GROUPS // 2), :, cols_of(g, 0)] + pair_in[g - 1]
        ref = pair_slots.at[g - 1, chip]
        for d in far_first:
            pltpu.make_async_remote_copy(
                src_ref=ref, dst_ref=ref, send_sem=slot_s, recv_sem=slot_r.at[g],
                **device(at(chip + d) * 2 + core),
            ).start()

    def scale_copy(g, h):
        ref = scales[g // (GROUPS // 2)].at[:, cols_of(g, h)]
        return pltpu.make_async_remote_copy(
            src_ref=ref, dst_ref=ref, send_sem=scale_s, recv_sem=scale_r.at[g],
            **device(partner),
        )

    def total(g):
        mine = slots if g == 0 else pair_slots.at[g - 1]
        count = mine.shape[0]
        take(mine.at[pl.ds(0, count - 1)], slot_r.at[g])
        acc = mine[0]
        for r in range(1, count):
            acc = acc + mine[r]
        scales[g // (GROUPS // 2)][:, cols_of(g, 0)] = acc / D_MODEL
        scale_copy(g, 0).start()

    def rows_of(offset, first=0, count=rows):
        start = (at(chip + offset) * 2 + core) * rows + first
        return pl.ds(pl.multiple_of(start, SLICE), count)

    def place(offset, q, p=None, first=0, count=rows):
        if p is None:
            return outs[q].at[rows_of(offset, first, count)]
        return outs[q].at[rows_of(offset, first, count), cols_of(p // 2, p % 2)]

    def neighbour(way):
        return device(at(chip + 1 - 2 * way) * 2 + core)

    def onward(ref, way, recv_sem, send_sem=None):
        return pltpu.make_async_remote_copy(
            src_ref=ref, dst_ref=ref, send_sem=ring_s.at[way] if send_sem is None else send_sem,
            recv_sem=recv_sem, **neighbour(way),
        )

    def raw_copy(i, way):
        some = pl.ds(i * SLICE, SLICE)
        return pltpu.make_async_remote_copy(
            src_ref=plain.at[0, some, cols_of(0, 0)], dst_ref=raw_in.at[way, some],
            send_sem=raw_s, recv_sem=raw_r.at[way], **neighbour(way),
        )

    def send_raw(i):
        if i < RAW // SLICE:
            for way in range(2):
                raw_copy(i, way).start()

    def side_copy(ref):
        return pltpu.make_async_remote_copy(
            src_ref=ref, dst_ref=ref, send_sem=side_s, recv_sem=side_r, **device(partner)
        )

    def narrow(p):
        g, h = p // 2, p % 2
        q = g // (GROUPS // 2)
        first = start_of(g, h)
        start = pl.multiple_of(me * rows, rows)

        @pl.loop(0, half // 128)
        def _(j):
            cols = pl.ds(pl.multiple_of(first + j * 128, 128), 128)
            inverse = 1.0 / scales[q][:, cols]
            outs[q][pl.ds(start, rows), cols] = (plain[q, :, cols] * inverse).astype(BF16)

    def send_own(p):
        narrow(p)
        q = p * 2 // PIECES
        for way in range(2):
            if p == 0:
                onward(place(0, q, p, RAW, rows - RAW), way, rest_r.at[way], rest_s).start()
            else:
                onward(place(0, q, p), way, ring_r.at[way, 0, q]).start()
        side_copy(place(0, q, p)).start()

    each = 2 * chunks // GROUPS
    for n in range(each):
        update(n)
    pl.semaphore_wait(barrier, 2 * CHIPS - 1)
    send_first()
    send_raw(0)
    for g in range(1, GROUPS):
        for n in range(g * each, (g + 1) * each):
            update(n)
        pair_copy(g).start()
        if g > 1:
            send_pair(g - 1)
            send_raw(g - 1)
    send_pair(GROUPS - 1)
    total(0)
    send_own(0)
    scale_copy(0, 1).wait_recv()
    send_own(1)
    for g in range(1, GROUPS):
        total(g)
        send_own(2 * g)
        scale_copy(g, 1).wait_recv()
        send_own(2 * g + 1)
    def scale_raw(way):
        take(raw_in.at[way, pl.ds(0, RAW)], raw_r.at[way])
        take(place(0, 0, 0, RAW, rows - RAW), rest_r.at[way])

        @pl.loop(0, half // 128)
        def _(j):
            here = pl.ds(pl.multiple_of(j * 128, 128), 128)
            cols = pl.ds(pl.multiple_of(start_of(0, 0) + j * 128, 128), 128)
            inverse = 1.0 / scale_g[:, cols]
            out_g[rows_of(2 * way - 1, 0, RAW), cols] = (
                raw_in[way, pl.ds(0, RAW), here] * inverse
            ).astype(BF16)

    steps = CHIPS // 2
    for step in range(steps - 1):
        for q in range(2):
            for way in range(2):
                offset = (2 * way - 1) * (step + 1)
                whole = place(offset, q)
                if step == 0 and q == 0:
                    scale_raw(way)
                    take(outs[q].at[rows_of(offset), pl.ds(0, width - half)], ring_r.at[way, step, q])
                else:
                    take(whole, ring_r.at[way, step, q])
                if step + 1 < steps - 1:
                    onward(whole, way, ring_r.at[way, step + 1, q]).start()
                elif q == way:
                    for i in range(PIECES // 2):
                        onward(place(offset, q, q * PIECES // 2 + i), way, last_r.at[way, i]).start()
                side_copy(whole).start()
    for i in range(PIECES // 2):
        for way in range(2):
            ref = place(steps, way, way * PIECES // 2 + i)
            take(ref, last_r.at[way, i])
            side_copy(ref).start()
    take(out_g, side_r)
    take(out_g, side_s)
    sent = out_g.at[pl.ds(0, rows * (CHIPS - 1) - rows * half // width)]
    for way in range(2):
        take(sent, ring_s.at[way])
    take(raw_in.at[:, pl.ds(0, RAW)], raw_s)
    take(out_g.at[pl.ds(0, 2 * (rows - RAW)), pl.ds(0, half)], rest_s)
    take(scale_g.at[:, pl.ds(0, half * GROUPS)], scale_s)
    take(slots.at[pl.ds(0, 2 * CHIPS - 1)], slot_s)
    take(pair_slots.at[:, pl.ds(0, CHIPS - 1)], slot_s)
    take(pair_in, pair_s)


def write_kernel(g, u, a, b, g_out, u_out, a_out, b_out, sem):
    parts = 16
    rows = g.shape[0] // parts
    copies = []
    for k in range(parts):
        where = pl.ds(k * rows, rows)
        copies.append(pltpu.make_async_copy(g.at[where], g_out.at[where], sem))
        copies.append(pltpu.make_async_copy(u.at[where], u_out.at[where], sem))
    copies.append(pltpu.make_async_copy(a, a_out, sem))
    copies.append(pltpu.make_async_copy(b, b_out, sem))
    for copy in copies:
        copy.start()
    for copy in copies:
        copy.wait()


def shards(weight_gate, moment_gate, square_gate, weight_up, moment_up, square_up, norm_gain):
    rows, width = weight_gate.shape
    total_rows = rows * lax.axis_size("rows")
    any_spec = pl.BlockSpec(memory_space=pl.ANY)
    hbm_spec = pl.BlockSpec(memory_space=pltpu.HBM)
    vmem_spec = pl.BlockSpec(memory_space=pltpu.VMEM)
    dma = pltpu.SemaphoreType.DMA
    g, u, a, b = pl.pallas_call(
        gather_kernel,
        name="gather",
        out_shape=(
            pltpu.VMEM((total_rows, width), BF16),
            pltpu.VMEM((total_rows, width), BF16),
            pltpu.VMEM((1, width), F32),
            pltpu.VMEM((1, width), F32),
        ),
        in_specs=[hbm_spec] * 7,
        out_specs=(vmem_spec,) * 4,
        scratch_shapes=[
            pltpu.VMEM((2, 3, rows, width), F32),
            pltpu.VMEM((2, rows, width), F32),
            pltpu.VMEM((1, rows), F32),
            pltpu.VMEM((rows, rows), F32),
            pltpu.VMEM((2, 1, width), F32),
            pltpu.VMEM((2 * CHIPS, 1, width // GROUPS), F32),
            pltpu.VMEM((GROUPS - 1, 1, width // GROUPS), F32),
            pltpu.VMEM((GROUPS - 1, CHIPS, 1, width // GROUPS), F32),
            pltpu.VMEM((2, RAW, width // GROUPS), F32),
            dma((AHEAD + 1,)), dma,
            dma, dma((GROUPS - 1,)), dma, dma((GROUPS,)), dma, dma((GROUPS,)),
            dma, dma((2,)), dma, dma((2,)),
            dma((2,)), dma((2, CHIPS // 2 - 1, 2)), dma((2, PIECES // 2)), dma, dma,
        ],
        compiler_params=pltpu.CompilerParams(
            collective_id=0, has_side_effects=True, vmem_limit_bytes=47 * 2**20
        ),
    )(weight_gate, moment_gate, square_gate, weight_up, moment_up, square_up, norm_gain.reshape(1, rows))
    g, u, a, b = pl.pallas_call(
        write_kernel,
        name="write",
        out_shape=(
            jax.ShapeDtypeStruct((total_rows, width), BF16),
            jax.ShapeDtypeStruct((total_rows, width), BF16),
            jax.ShapeDtypeStruct((1, width), F32),
            jax.ShapeDtypeStruct((1, width), F32),
        ),
        in_specs=[vmem_spec] * 4,
        out_specs=(any_spec,) * 4,
        scratch_shapes=[dma],
        compiler_params=pltpu.CompilerParams(vmem_limit_bytes=2 * 2**20),
    )(g, u, a, b)
    return g, u, a.reshape(width), b.reshape(width)


def solution(mesh):
    return jax.shard_map(
        shards,
        mesh=mesh,
        in_specs=(
            P(("trial", "rows"), "cols"),
            P(("trial", "rows"), "cols"),
            P(("trial", "rows"), "cols"),
            P(("trial", "rows"), "cols"),
            P(("trial", "rows"), "cols"),
            P(("trial", "rows"), "cols"),
            P(("trial", "rows")),
        ),
        out_specs=(
            P("trial", "cols"),
            P("trial", "cols"),
            P(("trial", "cols")),
            P(("trial", "cols")),
        ),
        check_vma=False,
    )
```

```python
import functools

import jax
import jax.numpy as jnp
from jax import lax
from jax.experimental import pallas as pl
from jax.experimental.pallas import tpu as pltpu
from jax.sharding import PartitionSpec as P

D_MODEL = 2048
learn_rate = 0.02
decay_rate = 0.05
tiny_value = 1e-08

MESH = pl.DeviceIdType.MESH
F32, BF16 = jnp.float32, jnp.bfloat16

CHIPS = 8
GROUPS = 4
PIECES = 8
CHUNK = 512
AHEAD = 3
RAW = 64
SLICES = ((0,), (1,), (), ())
SLICE = 32


def gather_kernel(
    wg, mg, sg, wu, mu, su, gain_hbm,
    out_g, out_u, scale_g, scale_u,
    held, plain, gain, gain_t, part, slots, pair_in, pair_slots, raw_in,
    load_sem, gain_sem, pair_s, pair_r, slot_s, slot_r, scale_s, scale_r,
    raw_s, raw_r, rest_s, rest_r, ring_s, ring_r, last_r, side_s, side_r,
):
    rows, width = wg.shape
    wide = width * 2 // GROUPS
    half = wide // 2
    chunks = width // CHUNK
    me = lax.axis_index("rows")
    chip, core = me // 2, me % 2
    partner = chip * 2 + (1 - core)
    outs, scales = (out_g, out_u), (scale_g, scale_u)
    sources = ((wg, mg, sg), (wu, mu, su))

    def at(c):
        return lax.rem(c + CHIPS, CHIPS)

    def device(r):
        return dict(device_id={"rows": r}, device_id_type=MESH)

    def take(ref, sem):
        pltpu.make_async_copy(ref, ref, sem).wait()

    def load(n):
        q, k = n // chunks, n % chunks
        cols = pl.ds(k * CHUNK, CHUNK)
        for i in range(3):
            pltpu.make_async_copy(
                sources[q][i].at[:, cols], held.at[q, i, :, cols], load_sem.at[n % (AHEAD + 1)]
            ).start()

    gain_copy = pltpu.make_async_copy(gain_hbm, gain, gain_sem)
    gain_copy.start()
    for n in range(AHEAD):
        load(n)

    barrier = pltpu.get_barrier_semaphore()
    for d in (4, 3, 5, 2, 6, 1, 7):
        for h in range(2):
            pl.semaphore_signal(barrier, inc=1, **device(at(chip + d) * 2 + h))
    pl.semaphore_signal(barrier, inc=1, **device(partner))

    gain_copy.wait()
    gain_t[...] = jnp.broadcast_to(gain[...], (rows, rows)).T

    def update(n):
        q, k = n // chunks, n % chunks
        if n + AHEAD < 2 * chunks:
            load(n + AHEAD)
        block = held.at[q, :, :, pl.ds(k * CHUNK, CHUNK)]
        pltpu.make_async_copy(block, block, load_sem.at[n % (AHEAD + 1)]).wait()

        @pl.loop(k * CHUNK // 128, (k + 1) * CHUNK // 128)
        def _(j):
            cols = pl.ds(pl.multiple_of(j * 128, 128), 128)
            w = held[q, 0, :, cols]
            m = held[q, 1, :, cols]
            s = held[q, 2, :, cols]
            whole = w - learn_rate * (m / (jnp.sqrt(s) + tiny_value) + decay_rate * w)
            gained = whole * gain_t[...]
            plain[q, :, cols] = gained
            part[q, :, cols] = jnp.sum(jnp.abs(gained), axis=0, keepdims=True)

    def start_of(g, h):
        return (g % (GROUPS // 2)) * wide + (core + h) % 2 * half

    def cols_of(g, h):
        return pl.ds(pl.multiple_of(start_of(g, h), half), half)

    far_first = (4, 3, 5, 2, 6, 1, 7)

    def part_of(g, where):
        return part.at[g // (GROUPS // 2), :, where]

    def first_copy(where, target):
        return pltpu.make_async_remote_copy(
            src_ref=part_of(0, where), dst_ref=slots.at[me],
            send_sem=slot_s, recv_sem=slot_r.at[0], **device(target),
        )

    def send_first():
        for d in far_first:
            for h in range(2):
                first_copy(pl.ds(h * half, half), at(chip + d) * 2 + h).start()
        first_copy(cols_of(0, 1), partner).start()
        slots[me] = part[0, :, cols_of(0, 0)]

    rest = range(1, GROUPS)

    def pair_copy(g):
        return pltpu.make_async_remote_copy(
            src_ref=part_of(g, cols_of(g, 1)), dst_ref=pair_in.at[g - 1],
            send_sem=pair_s, recv_sem=pair_r, **device(partner),
        )

    def send_rest():
        take(pair_in, pair_r)
        for g in rest:
            pair_slots[chip, g - 1] = part_of(g, cols_of(g, 0))[...] + pair_in[g - 1]
        ref = pair_slots.at[chip]
        for d in far_first:
            pltpu.make_async_remote_copy(
                src_ref=ref, dst_ref=ref, send_sem=slot_s, recv_sem=slot_r.at[1],
                **device(at(chip + d) * 2 + core),
            ).start()

    def scale_copy(g):
        ref = scales[g // (GROUPS // 2)].at[:, cols_of(g, 0)]
        return pltpu.make_async_remote_copy(
            src_ref=ref, dst_ref=ref, send_sem=scale_s, recv_sem=scale_r.at[min(g, 1)],
            **device(partner),
        )

    def total_first():
        take(slots.at[pl.ds(0, 2 * CHIPS - 1)], slot_r.at[0])
        acc = slots[0]
        for r in range(1, 2 * CHIPS):
            acc = acc + slots[r]
        scale_g[:, cols_of(0, 0)] = acc / D_MODEL
        scale_copy(0).start()

    def total_rest():
        take(pair_slots.at[pl.ds(0, CHIPS - 1)], slot_r.at[1])
        for g in rest:
            acc = pair_slots[0, g - 1]
            for r in range(1, CHIPS):
                acc = acc + pair_slots[r, g - 1]
            scales[g // (GROUPS // 2)][:, cols_of(g, 0)] = acc / D_MODEL
            scale_copy(g).start()

    def rows_of(offset, first=0, count=rows):
        start = (at(chip + offset) * 2 + core) * rows + first
        return pl.ds(pl.multiple_of(start, SLICE), count)

    def place(offset, g):
        cols = pl.ds((g % (GROUPS // 2)) * wide, wide)
        return outs[g * 2 // GROUPS].at[rows_of(offset), cols]

    def quarter(offset, g, i):
        cols = pl.ds((g % (GROUPS // 2)) * wide + i * half, half)
        return outs[g * 2 // GROUPS].at[rows_of(offset), cols]

    def neighbour(way):
        return device(at(chip + 1 - 2 * way) * 2 + core)

    def onward(ref, way, recv_sem, send_sem=None):
        return pltpu.make_async_remote_copy(
            src_ref=ref, dst_ref=ref, send_sem=ring_s.at[way] if send_sem is None else send_sem,
            recv_sem=recv_sem, **neighbour(way),
        )

    def raw_copy(i, way):
        some = pl.ds(i * SLICE, SLICE)
        return pltpu.make_async_remote_copy(
            src_ref=plain.at[0, some, cols_of(0, 0)], dst_ref=raw_in.at[way, some],
            send_sem=raw_s, recv_sem=raw_r.at[way], **neighbour(way),
        )

    def send_raw(turn):
        for i in SLICES[turn]:
            for way in range(2):
                raw_copy(i, way).start()

    def side_copy(ref):
        return pltpu.make_async_remote_copy(
            src_ref=ref, dst_ref=ref, send_sem=side_s, recv_sem=side_r, **device(partner)
        )

    def narrow(p):
        g, h = p // 2, p % 2
        q = g // (GROUPS // 2)
        first = start_of(g, h)
        start = pl.multiple_of(me * rows, rows)

        @pl.loop(0, half // 128)
        def _(j):
            cols = pl.ds(pl.multiple_of(first + j * 128, 128), 128)
            inverse = 1.0 / scales[q][:, cols]
            outs[q][pl.ds(start, rows), cols] = (plain[q, :, cols] * inverse).astype(BF16)

    def send_way(p, way):
        g = p // 2
        if p == 0:
            ref = outs[0].at[rows_of(0, RAW, rows - RAW), cols_of(0, 0)]
            onward(ref, way, rest_r.at[way], rest_s).start()
        else:
            ref = outs[g * 2 // GROUPS].at[rows_of(0), cols_of(g, p % 2)]
            onward(ref, way, ring_r.at[way, 0, g]).start()

    def send_own(p):
        g = p // 2
        narrow(p)
        send_way(p, 0)
        if g != late:
            send_way(p, 1)
        side_copy(outs[g * 2 // GROUPS].at[rows_of(0), cols_of(g, p % 2)]).start()

    late = 1
    orders = ((0, 1, 2, 3), (0, 2, 3, 1))
    each = 2 * chunks // GROUPS
    for n in range(each):
        update(n)
    pl.semaphore_wait(barrier, 2 * CHIPS - 1)
    send_first()
    send_raw(0)
    for g in rest:
        for n in range(g * each, (g + 1) * each):
            update(n)
        pair_copy(g).start()
        send_raw(g)
    send_rest()
    total_first()
    send_own(0)
    take(scale_g.at[:, cols_of(0, 0)], scale_r.at[0])
    send_own(1)
    total_rest()
    send_own(2)
    take(scale_g.at[:, pl.ds(0, half * (GROUPS - 1))], scale_r.at[1])
    for p in range(3, PIECES):
        send_own(p)
    for h in range(2):
        send_way(2 * late + h, 1)
    def scale_raw(way):
        take(raw_in.at[way, pl.ds(0, RAW)], raw_r.at[way])
        take(out_g.at[pl.ds(0, rows - RAW), pl.ds(0, half)], rest_r.at[way])

        @pl.loop(0, half // 128)
        def _(j):
            here = pl.ds(pl.multiple_of(j * 128, 128), 128)
            cols = pl.ds(pl.multiple_of(start_of(0, 0) + j * 128, 128), 128)
            inverse = 1.0 / scale_g[:, cols]
            out_g[rows_of(2 * way - 1, 0, RAW), cols] = (
                raw_in[way, pl.ds(0, RAW), here] * inverse
            ).astype(BF16)

    steps = CHIPS // 2
    farthest = ((0, 1), (2, 3))
    for step in range(steps - 1):
        for turn in range(GROUPS):
            for way in range(2):
                g = orders[way][turn]
                offset = (2 * way - 1) * (step + 1)
                whole = place(offset, g)
                if step == 0 and g == 0:
                    scale_raw(way)
                    take(quarter(offset, g, 0), ring_r.at[way, step, g])
                else:
                    take(whole, ring_r.at[way, step, g])
                if step + 1 < steps - 1:
                    onward(whole, way, ring_r.at[way, step + 1, g]).start()
                elif g in farthest[way]:
                    for i in range(2):
                        k = farthest[way].index(g) * 2 + i
                        onward(quarter(offset, g, i), way, last_r.at[way, k]).start()
                side_copy(whole).start()
    for k in range(PIECES // 2):
        for way in range(2):
            ref = quarter(steps, farthest[way][k // 2], k % 2)
            take(ref, last_r.at[way, k])
            side_copy(ref).start()
    take(out_g, side_r)
    take(out_g, side_s)
    sent = out_g.at[pl.ds(0, rows * (CHIPS - 1) - rows * half // width)]
    for way in range(2):
        take(sent, ring_s.at[way])
    take(raw_in.at[:, pl.ds(0, RAW)], raw_s)
    take(out_g.at[pl.ds(0, 2 * (rows - RAW)), pl.ds(0, half)], rest_s)
    take(scale_g.at[:, pl.ds(0, half * GROUPS)], scale_s)
    take(slots.at[pl.ds(0, 2 * CHIPS - 1)], slot_s)
    take(pair_slots.at[pl.ds(0, CHIPS - 1)], slot_s)
    take(pair_in, pair_s)


def write_kernel(g, u, a, b, g_out, u_out, a_out, b_out, sem):
    parts = 16
    rows = g.shape[0] // parts
    copies = []
    for k in range(parts):
        where = pl.ds(k * rows, rows)
        copies.append(pltpu.make_async_copy(g.at[where], g_out.at[where], sem))
        copies.append(pltpu.make_async_copy(u.at[where], u_out.at[where], sem))
    copies.append(pltpu.make_async_copy(a, a_out, sem))
    copies.append(pltpu.make_async_copy(b, b_out, sem))
    for copy in copies:
        copy.start()
    for copy in copies:
        copy.wait()


def shards(weight_gate, moment_gate, square_gate, weight_up, moment_up, square_up, norm_gain):
    rows, width = weight_gate.shape
    total_rows = rows * lax.axis_size("rows")
    any_spec = pl.BlockSpec(memory_space=pl.ANY)
    hbm_spec = pl.BlockSpec(memory_space=pltpu.HBM)
    vmem_spec = pl.BlockSpec(memory_space=pltpu.VMEM)
    dma = pltpu.SemaphoreType.DMA
    g, u, a, b = pl.pallas_call(
        gather_kernel,
        name="gather",
        out_shape=(
            pltpu.VMEM((total_rows, width), BF16),
            pltpu.VMEM((total_rows, width), BF16),
            pltpu.VMEM((1, width), F32),
            pltpu.VMEM((1, width), F32),
        ),
        in_specs=[hbm_spec] * 7,
        out_specs=(vmem_spec,) * 4,
        scratch_shapes=[
            pltpu.VMEM((2, 3, rows, width), F32),
            pltpu.VMEM((2, rows, width), F32),
            pltpu.VMEM((1, rows), F32),
            pltpu.VMEM((rows, rows), F32),
            pltpu.VMEM((2, 1, width), F32),
            pltpu.VMEM((2 * CHIPS, 1, width // GROUPS), F32),
            pltpu.VMEM((GROUPS - 1, 1, width // GROUPS), F32),
            pltpu.VMEM((CHIPS, GROUPS - 1, 1, width // GROUPS), F32),
            pltpu.VMEM((2, RAW, width // GROUPS), F32),
            dma((AHEAD + 1,)), dma,
            dma, dma, dma, dma((2,)), dma, dma((2,)),
            dma, dma((2,)), dma, dma((2,)),
            dma((2,)), dma((2, CHIPS // 2 - 1, GROUPS)), dma((2, PIECES // 2)), dma, dma,
        ],
        compiler_params=pltpu.CompilerParams(
            collective_id=0, has_side_effects=True, vmem_limit_bytes=47 * 2**20
        ),
    )(weight_gate, moment_gate, square_gate, weight_up, moment_up, square_up, norm_gain.reshape(1, rows))
    g, u, a, b = pl.pallas_call(
        write_kernel,
        name="write",
        out_shape=(
            jax.ShapeDtypeStruct((total_rows, width), BF16),
            jax.ShapeDtypeStruct((total_rows, width), BF16),
            jax.ShapeDtypeStruct((1, width), F32),
            jax.ShapeDtypeStruct((1, width), F32),
        ),
        in_specs=[vmem_spec] * 4,
        out_specs=(any_spec,) * 4,
        scratch_shapes=[dma],
        compiler_params=pltpu.CompilerParams(vmem_limit_bytes=2 * 2**20),
    )(g, u, a, b)
    return g, u, a.reshape(width), b.reshape(width)


def solution(mesh):
    return jax.shard_map(
        shards,
        mesh=mesh,
        in_specs=(
            P(("trial", "rows"), "cols"),
            P(("trial", "rows"), "cols"),
            P(("trial", "rows"), "cols"),
            P(("trial", "rows"), "cols"),
            P(("trial", "rows"), "cols"),
            P(("trial", "rows"), "cols"),
            P(("trial", "rows")),
        ),
        out_specs=(
            P("trial", "cols"),
            P("trial", "cols"),
            P(("trial", "cols")),
            P(("trial", "cols")),
        ),
        check_vma=False,
    )
```

```python
import functools

import jax
import jax.numpy as jnp
from jax import lax
from jax.experimental import pallas as pl
from jax.experimental.pallas import tpu as pltpu
from jax.sharding import PartitionSpec as P

D_MODEL = 2048
learn_rate = 0.02
decay_rate = 0.05
tiny_value = 1e-08

MESH = pl.DeviceIdType.MESH
F32, BF16 = jnp.float32, jnp.bfloat16

CHIPS = 8
GROUPS = 4
PIECES = 8
CHUNK = 512
AHEAD = 3
RAW = 64
SLICES = ((0,), (1,), (), ())
SLICE = 32


def gather_kernel(
    wg, mg, sg, wu, mu, su, gain_hbm,
    out_g, out_u, scale_g, scale_u,
    held, plain, gain, gain_t, part, slots, pair_in, pair_slots, raw_in,
    load_sem, gain_sem, sent, pair_r, slot_r, scale_r, raw_r, rest_r, ring_r, last_r, side_r,
):
    rows, width = wg.shape
    wide = width * 2 // GROUPS
    half = wide // 2
    chunks = width // CHUNK
    me = lax.axis_index("rows")
    chip, core = me // 2, me % 2
    partner = chip * 2 + (1 - core)
    outs, scales = (out_g, out_u), (scale_g, scale_u)
    sources = ((wg, mg, sg), (wu, mu, su))

    def at(c):
        return lax.rem(c + CHIPS, CHIPS)

    def device(r):
        return dict(device_id={"rows": r}, device_id_type=MESH)

    def take(ref, sem):
        pltpu.make_async_copy(ref, ref, sem).wait()

    def load(n):
        q, k = n // chunks, n % chunks
        cols = pl.ds(k * CHUNK, CHUNK)
        for i in range(3):
            pltpu.make_async_copy(
                sources[q][i].at[:, cols], held.at[q, i, :, cols], load_sem.at[n % (AHEAD + 1)]
            ).start()

    gain_copy = pltpu.make_async_copy(gain_hbm, gain, gain_sem)
    gain_copy.start()
    for n in range(AHEAD):
        load(n)

    barrier = pltpu.get_barrier_semaphore()
    for d in (4, 3, 5, 2, 6, 1, 7):
        for h in range(2):
            pl.semaphore_signal(barrier, inc=1, **device(at(chip + d) * 2 + h))
    pl.semaphore_signal(barrier, inc=1, **device(partner))

    gain_copy.wait()
    gain_t[...] = jnp.broadcast_to(gain[...], (rows, rows)).T

    def update(n):
        q, k = n // chunks, n % chunks
        if n + AHEAD < 2 * chunks:
            load(n + AHEAD)
        block = held.at[q, :, :, pl.ds(k * CHUNK, CHUNK)]
        pltpu.make_async_copy(block, block, load_sem.at[n % (AHEAD + 1)]).wait()

        @pl.loop(k * CHUNK // 128, (k + 1) * CHUNK // 128)
        def _(j):
            cols = pl.ds(pl.multiple_of(j * 128, 128), 128)
            w = held[q, 0, :, cols]
            m = held[q, 1, :, cols]
            s = held[q, 2, :, cols]
            whole = w - learn_rate * (m / (jnp.sqrt(s) + tiny_value) + decay_rate * w)
            gained = whole * gain_t[...]
            plain[q, :, cols] = gained
            part[q, :, cols] = jnp.sum(jnp.abs(gained), axis=0, keepdims=True)

    def start_of(g, h):
        return (g % (GROUPS // 2)) * wide + (core + h) % 2 * half

    def cols_of(g, h):
        return pl.ds(pl.multiple_of(start_of(g, h), half), half)

    far_first = (4, 3, 5, 2, 6, 1, 7)

    def part_of(g, where):
        return part.at[g // (GROUPS // 2), :, where]

    def first_copy(where, target):
        return pltpu.make_async_remote_copy(
            src_ref=part_of(0, where), dst_ref=slots.at[me],
            send_sem=sent, recv_sem=slot_r.at[0], **device(target),
        )

    def send_first():
        for d in far_first:
            for h in range(2):
                first_copy(pl.ds(h * half, half), at(chip + d) * 2 + h).start()
        first_copy(cols_of(0, 1), partner).start()
        slots[me] = part[0, :, cols_of(0, 0)]

    rest = range(1, GROUPS)

    def pair_copy(g):
        return pltpu.make_async_remote_copy(
            src_ref=part_of(g, cols_of(g, 1)), dst_ref=pair_in.at[g - 1],
            send_sem=sent, recv_sem=pair_r, **device(partner),
        )

    def send_rest():
        take(pair_in, pair_r)
        for g in rest:
            pair_slots[chip, g - 1] = part_of(g, cols_of(g, 0))[...] + pair_in[g - 1]
        ref = pair_slots.at[chip]
        for d in far_first:
            pltpu.make_async_remote_copy(
                src_ref=ref, dst_ref=ref, send_sem=sent, recv_sem=slot_r.at[1],
                **device(at(chip + d) * 2 + core),
            ).start()

    def scale_copy(g):
        ref = scales[g // (GROUPS // 2)].at[:, cols_of(g, 0)]
        return pltpu.make_async_remote_copy(
            src_ref=ref, dst_ref=ref, send_sem=sent, recv_sem=scale_r.at[min(g, 1)],
            **device(partner),
        )

    def total_first():
        take(slots.at[pl.ds(0, 2 * CHIPS - 1)], slot_r.at[0])
        acc = slots[0]
        for r in range(1, 2 * CHIPS):
            acc = acc + slots[r]
        scale_g[:, cols_of(0, 0)] = acc / D_MODEL
        scale_copy(0).start()

    def total_rest():
        take(pair_slots.at[pl.ds(0, CHIPS - 1)], slot_r.at[1])
        for g in rest:
            acc = pair_slots[0, g - 1]
            for r in range(1, CHIPS):
                acc = acc + pair_slots[r, g - 1]
            scales[g // (GROUPS // 2)][:, cols_of(g, 0)] = acc / D_MODEL
            scale_copy(g).start()

    def rows_of(offset, first=0, count=rows):
        start = (at(chip + offset) * 2 + core) * rows + first
        return pl.ds(pl.multiple_of(start, SLICE), count)

    def place(offset, g):
        cols = pl.ds((g % (GROUPS // 2)) * wide, wide)
        return outs[g * 2 // GROUPS].at[rows_of(offset), cols]

    def quarter(offset, g, i):
        cols = pl.ds((g % (GROUPS // 2)) * wide + i * half, half)
        return outs[g * 2 // GROUPS].at[rows_of(offset), cols]

    def neighbour(way):
        return device(at(chip + 1 - 2 * way) * 2 + core)

    def onward(ref, way, recv_sem):
        return pltpu.make_async_remote_copy(
            src_ref=ref, dst_ref=ref, send_sem=sent, recv_sem=recv_sem, **neighbour(way)
        )

    def raw_copy(i, way):
        some = pl.ds(i * SLICE, SLICE)
        return pltpu.make_async_remote_copy(
            src_ref=plain.at[0, some, cols_of(0, 0)], dst_ref=raw_in.at[way, some],
            send_sem=sent, recv_sem=raw_r.at[way], **neighbour(way),
        )

    def send_raw(turn):
        for i in SLICES[turn]:
            for way in range(2):
                raw_copy(i, way).start()

    def side_copy(ref):
        return pltpu.make_async_remote_copy(
            src_ref=ref, dst_ref=ref, send_sem=sent, recv_sem=side_r, **device(partner)
        )

    def narrow(p):
        g, h = p // 2, p % 2
        q = g // (GROUPS // 2)
        first = start_of(g, h)
        start = pl.multiple_of(me * rows, rows)

        @pl.loop(0, half // 128)
        def _(j):
            cols = pl.ds(pl.multiple_of(first + j * 128, 128), 128)
            inverse = 1.0 / scales[q][:, cols]
            outs[q][pl.ds(start, rows), cols] = (plain[q, :, cols] * inverse).astype(BF16)

    def unit_of(g, way):
        return orders[way].index(g) // 2

    def send_way(p, way):
        g = p // 2
        if p == 0:
            ref = outs[0].at[rows_of(0, RAW, rows - RAW), cols_of(0, 0)]
            onward(ref, way, rest_r.at[way]).start()
        else:
            ref = outs[g * 2 // GROUPS].at[rows_of(0), cols_of(g, p % 2)]
            onward(ref, way, ring_r.at[way, 0, unit_of(g, way)]).start()

    def send_own(p):
        g = p // 2
        narrow(p)
        send_way(p, 0)
        if g != late:
            send_way(p, 1)
        side_copy(outs[g * 2 // GROUPS].at[rows_of(0), cols_of(g, p % 2)]).start()

    late = 1
    orders = ((0, 1, 2, 3), (0, 2, 3, 1))
    each = 2 * chunks // GROUPS
    for n in range(each):
        update(n)
    pl.semaphore_wait(barrier, 2 * CHIPS - 1)
    send_first()
    send_raw(0)
    for g in rest:
        for n in range(g * each, (g + 1) * each):
            update(n)
        pair_copy(g).start()
        send_raw(g)
    send_rest()
    total_first()
    send_own(0)
    take(scale_g.at[:, cols_of(0, 0)], scale_r.at[0])
    send_own(1)
    total_rest()
    send_own(2)
    take(scale_g.at[:, pl.ds(0, half * (GROUPS - 1))], scale_r.at[1])
    for p in range(3, PIECES):
        send_own(p)
    for h in range(2):
        send_way(2 * late + h, 1)
    def scale_raw(way):
        take(raw_in.at[way, pl.ds(0, RAW)], raw_r.at[way])
        take(out_g.at[pl.ds(0, rows - RAW), pl.ds(0, half)], rest_r.at[way])

        @pl.loop(0, half // 128)
        def _(j):
            here = pl.ds(pl.multiple_of(j * 128, 128), 128)
            cols = pl.ds(pl.multiple_of(start_of(0, 0) + j * 128, 128), 128)
            inverse = 1.0 / scale_g[:, cols]
            out_g[rows_of(2 * way - 1, 0, RAW), cols] = (
                raw_in[way, pl.ds(0, RAW), here] * inverse
            ).astype(BF16)

    steps = CHIPS // 2
    farthest = ((0, 1), (2, 3))
    for step in range(steps - 1):
        for unit in range(2):
            for way in range(2):
                offset = (2 * way - 1) * (step + 1)
                groups = orders[way][2 * unit : 2 * unit + 2]
                if step == 0 and unit == 0:
                    scale_raw(way)
                    take(out_g.at[pl.ds(0, rows), pl.ds(0, width - half)], ring_r.at[way, step, unit])
                else:
                    take(out_g.at[pl.ds(0, rows)], ring_r.at[way, step, unit])
                for g in groups:
                    if step + 1 < steps - 1:
                        onward(place(offset, g), way, ring_r.at[way, step + 1, unit]).start()
                    elif g in farthest[way]:
                        for i in range(2):
                            k = farthest[way].index(g) * 2 + i
                            onward(quarter(offset, g, i), way, last_r.at[way, k]).start()
                    side_copy(place(offset, g)).start()
    for k in range(PIECES // 2):
        for way in range(2):
            ref = quarter(steps, farthest[way][k // 2], k % 2)
            take(ref, last_r.at[way, k])
            side_copy(ref).start()
    take(out_g, side_r)
    take(out_g, sent)
    for way in range(2):
        take(out_g.at[pl.ds(0, rows * (CHIPS - 1) - rows * half // width)], sent)
    take(raw_in, sent)
    take(out_g.at[pl.ds(0, 2 * (rows - RAW)), pl.ds(0, half)], sent)
    take(scale_g.at[:, pl.ds(0, half * GROUPS)], sent)
    take(slots.at[pl.ds(0, 2 * CHIPS - 1)], sent)
    take(pair_slots.at[pl.ds(0, CHIPS - 1)], sent)
    take(pair_in, sent)


def write_kernel(g, u, a, b, g_out, u_out, a_out, b_out, sem):
    parts = 16
    rows = g.shape[0] // parts
    copies = []
    for k in range(parts):
        where = pl.ds(k * rows, rows)
        copies.append(pltpu.make_async_copy(g.at[where], g_out.at[where], sem))
        copies.append(pltpu.make_async_copy(u.at[where], u_out.at[where], sem))
    copies.append(pltpu.make_async_copy(a, a_out, sem))
    copies.append(pltpu.make_async_copy(b, b_out, sem))
    for copy in copies:
        copy.start()
    for copy in copies:
        copy.wait()


def shards(weight_gate, moment_gate, square_gate, weight_up, moment_up, square_up, norm_gain):
    rows, width = weight_gate.shape
    total_rows = rows * lax.axis_size("rows")
    any_spec = pl.BlockSpec(memory_space=pl.ANY)
    hbm_spec = pl.BlockSpec(memory_space=pltpu.HBM)
    vmem_spec = pl.BlockSpec(memory_space=pltpu.VMEM)
    dma = pltpu.SemaphoreType.DMA
    g, u, a, b = pl.pallas_call(
        gather_kernel,
        name="gather",
        out_shape=(
            pltpu.VMEM((total_rows, width), BF16),
            pltpu.VMEM((total_rows, width), BF16),
            pltpu.VMEM((1, width), F32),
            pltpu.VMEM((1, width), F32),
        ),
        in_specs=[hbm_spec] * 7,
        out_specs=(vmem_spec,) * 4,
        scratch_shapes=[
            pltpu.VMEM((2, 3, rows, width), F32),
            pltpu.VMEM((2, rows, width), F32),
            pltpu.VMEM((1, rows), F32),
            pltpu.VMEM((rows, rows), F32),
            pltpu.VMEM((2, 1, width), F32),
            pltpu.VMEM((2 * CHIPS, 1, width // GROUPS), F32),
            pltpu.VMEM((GROUPS - 1, 1, width // GROUPS), F32),
            pltpu.VMEM((CHIPS, GROUPS - 1, 1, width // GROUPS), F32),
            pltpu.VMEM((2, RAW, width // GROUPS), F32),
            dma((AHEAD + 1,)), dma, dma, dma, dma((2,)), dma((2,)), dma((2,)), dma((2,)),
            dma((2, CHIPS // 2 - 1, 2)), dma((2, PIECES // 2)), dma,
        ],
        compiler_params=pltpu.CompilerParams(
            collective_id=0, has_side_effects=True, vmem_limit_bytes=47 * 2**20
        ),
    )(weight_gate, moment_gate, square_gate, weight_up, moment_up, square_up, norm_gain.reshape(1, rows))
    g, u, a, b = pl.pallas_call(
        write_kernel,
        name="write",
        out_shape=(
            jax.ShapeDtypeStruct((total_rows, width), BF16),
            jax.ShapeDtypeStruct((total_rows, width), BF16),
            jax.ShapeDtypeStruct((1, width), F32),
            jax.ShapeDtypeStruct((1, width), F32),
        ),
        in_specs=[vmem_spec] * 4,
        out_specs=(any_spec,) * 4,
        scratch_shapes=[dma],
        compiler_params=pltpu.CompilerParams(vmem_limit_bytes=2 * 2**20),
    )(g, u, a, b)
    return g, u, a.reshape(width), b.reshape(width)


def solution(mesh):
    return jax.shard_map(
        shards,
        mesh=mesh,
        in_specs=(
            P(("trial", "rows"), "cols"),
            P(("trial", "rows"), "cols"),
            P(("trial", "rows"), "cols"),
            P(("trial", "rows"), "cols"),
            P(("trial", "rows"), "cols"),
            P(("trial", "rows"), "cols"),
            P(("trial", "rows")),
        ),
        out_specs=(
            P("trial", "cols"),
            P("trial", "cols"),
            P(("trial", "cols")),
            P(("trial", "cols")),
        ),
        check_vma=False,
    )
```

```python
import functools

import jax
import jax.numpy as jnp
from jax import lax
from jax.experimental import pallas as pl
from jax.experimental.pallas import tpu as pltpu
from jax.sharding import PartitionSpec as P

D_MODEL = 2048
learn_rate = 0.02
decay_rate = 0.05
tiny_value = 1e-08

MESH = pl.DeviceIdType.MESH
F32, BF16 = jnp.float32, jnp.bfloat16

CHIPS = 8
GROUPS = 4
PIECES = 8
CHUNK = 512
AHEAD = 3
RAW = 80
SLICES = ((0, 1, 2), (), (), (3, 4))
SLICE = 16


def gather_kernel(
    wg, mg, sg, wu, mu, su, gain_hbm,
    out_g, out_u, scale_g, scale_u,
    held, plain, gain, gain_t, part, slots, pair_in, pair_slots, raw_in,
    load_sem, gain_sem, sent, pair_r, slot_r, scale_r, raw_r, rest_r, ring_r, last_r, side_r,
):
    rows, width = wg.shape
    wide = width * 2 // GROUPS
    half = wide // 2
    chunks = width // CHUNK
    me = lax.axis_index("rows")
    chip, core = me // 2, me % 2
    partner = chip * 2 + (1 - core)
    outs, scales = (out_g, out_u), (scale_g, scale_u)
    sources = ((wg, mg, sg), (wu, mu, su))

    def at(c):
        return lax.rem(c + CHIPS, CHIPS)

    def device(r):
        return dict(device_id={"rows": r}, device_id_type=MESH)

    def take(ref, sem):
        pltpu.make_async_copy(ref, ref, sem).wait()

    def load(n):
        q, k = n // chunks, n % chunks
        cols = pl.ds(k * CHUNK, CHUNK)
        for i in range(3):
            pltpu.make_async_copy(
                sources[q][i].at[:, cols], held.at[q, i, :, cols], load_sem.at[n % (AHEAD + 1)]
            ).start()

    barrier = pltpu.get_barrier_semaphore()
    for d in (4, 3, 5, 2, 6, 1, 7):
        for h in range(2):
            pl.semaphore_signal(barrier, inc=1, **device(at(chip + d) * 2 + h))
    pl.semaphore_signal(barrier, inc=1, **device(partner))

    gain_copy = pltpu.make_async_copy(gain_hbm, gain, gain_sem)
    gain_copy.start()
    for n in range(AHEAD):
        load(n)

    gain_copy.wait()
    gain_t[...] = jnp.broadcast_to(gain[...], (rows, rows)).T

    def update(n):
        q, k = n // chunks, n % chunks
        if n + AHEAD < 2 * chunks:
            load(n + AHEAD)
        block = held.at[q, :, :, pl.ds(k * CHUNK, CHUNK)]
        pltpu.make_async_copy(block, block, load_sem.at[n % (AHEAD + 1)]).wait()

        @pl.loop(k * CHUNK // 128, (k + 1) * CHUNK // 128)
        def _(j):
            cols = pl.ds(pl.multiple_of(j * 128, 128), 128)
            w = held[q, 0, :, cols]
            m = held[q, 1, :, cols]
            s = held[q, 2, :, cols]
            whole = w - learn_rate * (m / (jnp.sqrt(s) + tiny_value) + decay_rate * w)
            gained = whole * gain_t[...]
            plain[q, :, cols] = gained
            part[q, :, cols] = jnp.sum(jnp.abs(gained), axis=0, keepdims=True)

    def start_of(g, h):
        return (g % (GROUPS // 2)) * wide + (core + h) % 2 * half

    def cols_of(g, h):
        return pl.ds(pl.multiple_of(start_of(g, h), half), half)

    far_first = (4, 3, 5, 2, 6, 1, 7)

    def part_of(g, where):
        return part.at[g // (GROUPS // 2), :, where]

    def first_copy(where, target):
        return pltpu.make_async_remote_copy(
            src_ref=part_of(0, where), dst_ref=slots.at[me],
            send_sem=sent, recv_sem=slot_r.at[0], **device(target),
        )

    def send_first():
        for d in far_first:
            for h in range(2):
                first_copy(pl.ds(h * half, half), at(chip + d) * 2 + h).start()
        first_copy(cols_of(0, 1), partner).start()
        slots[me] = part[0, :, cols_of(0, 0)]

    rest = range(1, GROUPS)

    def pair_copy(g):
        return pltpu.make_async_remote_copy(
            src_ref=part_of(g, cols_of(g, 1)), dst_ref=pair_in.at[g - 1],
            send_sem=sent, recv_sem=pair_r, **device(partner),
        )

    def send_rest():
        take(pair_in, pair_r)
        for g in rest:
            pair_slots[chip, g - 1] = part_of(g, cols_of(g, 0))[...] + pair_in[g - 1]
        ref = pair_slots.at[chip]
        for d in far_first:
            pltpu.make_async_remote_copy(
                src_ref=ref, dst_ref=ref, send_sem=sent, recv_sem=slot_r.at[1],
                **device(at(chip + d) * 2 + core),
            ).start()

    def scale_copy(g):
        ref = scales[g // (GROUPS // 2)].at[:, cols_of(g, 0)]
        return pltpu.make_async_remote_copy(
            src_ref=ref, dst_ref=ref, send_sem=sent, recv_sem=scale_r.at[min(g, 1)],
            **device(partner),
        )

    def total_first():
        take(slots.at[pl.ds(0, 2 * CHIPS - 1)], slot_r.at[0])
        acc = slots[0]
        for r in range(1, 2 * CHIPS):
            acc = acc + slots[r]
        scale_g[:, cols_of(0, 0)] = acc / D_MODEL
        scale_copy(0).start()

    def total_rest():
        take(pair_slots.at[pl.ds(0, CHIPS - 1)], slot_r.at[1])
        for g in rest:
            acc = pair_slots[0, g - 1]
            for r in range(1, CHIPS):
                acc = acc + pair_slots[r, g - 1]
            scales[g // (GROUPS // 2)][:, cols_of(g, 0)] = acc / D_MODEL
            scale_copy(g).start()

    def rows_of(offset, first=0, count=rows):
        start = (at(chip + offset) * 2 + core) * rows + first
        return pl.ds(pl.multiple_of(start, SLICE), count)

    def place(offset, g):
        cols = pl.ds((g % (GROUPS // 2)) * wide, wide)
        return outs[g * 2 // GROUPS].at[rows_of(offset), cols]

    def quarter(offset, g, i):
        cols = pl.ds((g % (GROUPS // 2)) * wide + i * half, half)
        return outs[g * 2 // GROUPS].at[rows_of(offset), cols]

    def neighbour(way):
        return device(at(chip + 1 - 2 * way) * 2 + core)

    def onward(ref, way, recv_sem):
        return pltpu.make_async_remote_copy(
            src_ref=ref, dst_ref=ref, send_sem=sent, recv_sem=recv_sem, **neighbour(way)
        )

    def raw_copy(i, way):
        some = pl.ds(i * SLICE, SLICE)
        return pltpu.make_async_remote_copy(
            src_ref=plain.at[0, some, cols_of(0, 0)], dst_ref=raw_in.at[way, some],
            send_sem=sent, recv_sem=raw_r.at[way], **neighbour(way),
        )

    def send_raw(turn):
        for i in SLICES[turn]:
            for way in range(2):
                raw_copy(i, way).start()

    def side_copy(ref):
        return pltpu.make_async_remote_copy(
            src_ref=ref, dst_ref=ref, send_sem=sent, recv_sem=side_r, **device(partner)
        )

    def narrow(p):
        g, h = p // 2, p % 2
        q = g // (GROUPS // 2)
        first = start_of(g, h)
        start = pl.multiple_of(me * rows, rows)

        @pl.loop(0, half // 128)
        def _(j):
            cols = pl.ds(pl.multiple_of(first + j * 128, 128), 128)
            inverse = 1.0 / scales[q][:, cols]
            outs[q][pl.ds(start, rows), cols] = (plain[q, :, cols] * inverse).astype(BF16)

    def unit_of(g, way):
        return orders[way].index(g) // 2

    def send_way(p, way):
        g = p // 2
        if p == 0:
            ref = outs[0].at[rows_of(0, RAW, rows - RAW), cols_of(0, 0)]
            onward(ref, way, rest_r.at[way]).start()
        else:
            ref = outs[g * 2 // GROUPS].at[rows_of(0), cols_of(g, p % 2)]
            onward(ref, way, ring_r.at[way, 0, unit_of(g, way)]).start()

    def send_own(p):
        g = p // 2
        narrow(p)
        send_way(p, 0)
        if g != late:
            send_way(p, 1)
        side_copy(outs[g * 2 // GROUPS].at[rows_of(0), cols_of(g, p % 2)]).start()

    late = 1
    orders = ((0, 1, 2, 3), (0, 2, 3, 1))
    each = 2 * chunks // GROUPS
    for n in range(each):
        update(n)
    pl.semaphore_wait(barrier, 2 * CHIPS - 1)
    send_first()
    send_raw(0)
    for g in rest:
        for n in range(g * each, (g + 1) * each):
            update(n)
        pair_copy(g).start()
        if g < GROUPS - 1:
            send_raw(g)
    send_rest()
    send_raw(GROUPS - 1)
    total_first()
    send_own(0)
    take(scale_g.at[:, cols_of(0, 0)], scale_r.at[0])
    send_own(1)
    total_rest()
    send_own(2)
    take(scale_g.at[:, pl.ds(0, half * (GROUPS - 1))], scale_r.at[1])
    for p in range(3, PIECES):
        send_own(p)
    for h in range(2):
        send_way(2 * late + h, 1)
    def scale_raw(way):
        take(raw_in.at[way, pl.ds(0, RAW)], raw_r.at[way])
        take(out_g.at[pl.ds(0, rows - RAW), pl.ds(0, half)], rest_r.at[way])

        @pl.loop(0, half // 128)
        def _(j):
            here = pl.ds(pl.multiple_of(j * 128, 128), 128)
            cols = pl.ds(pl.multiple_of(start_of(0, 0) + j * 128, 128), 128)
            inverse = 1.0 / scale_g[:, cols]
            out_g[rows_of(2 * way - 1, 0, RAW), cols] = (
                raw_in[way, pl.ds(0, RAW), here] * inverse
            ).astype(BF16)

    steps = CHIPS // 2
    farthest = ((0, 1), (2, 3))
    for step in range(steps - 1):
        for unit in range(2):
            for way in range(2):
                offset = (2 * way - 1) * (step + 1)
                groups = orders[way][2 * unit : 2 * unit + 2]
                if step == 0 and unit == 0:
                    scale_raw(way)
                    take(out_g.at[pl.ds(0, rows), pl.ds(0, width - half)], ring_r.at[way, step, unit])
                else:
                    take(out_g.at[pl.ds(0, rows)], ring_r.at[way, step, unit])
                for g in groups:
                    if step + 1 < steps - 1:
                        onward(place(offset, g), way, ring_r.at[way, step + 1, unit]).start()
                    elif g in farthest[way]:
                        for i in range(2):
                            k = farthest[way].index(g) * 2 + i
                            onward(quarter(offset, g, i), way, last_r.at[way, k]).start()
                    side_copy(place(offset, g)).start()
    for k in range(PIECES // 2):
        for way in range(2):
            ref = quarter(steps, farthest[way][k // 2], k % 2)
            take(ref, last_r.at[way, k])
            side_copy(ref).start()
    take(out_g, side_r)
    take(out_g, sent)
    for way in range(2):
        take(out_g.at[pl.ds(0, rows * (CHIPS - 1) - rows * half // width)], sent)
    take(raw_in, sent)
    take(out_g.at[pl.ds(0, 2 * (rows - RAW)), pl.ds(0, half)], sent)
    take(scale_g.at[:, pl.ds(0, half * GROUPS)], sent)
    take(slots.at[pl.ds(0, 2 * CHIPS - 1)], sent)
    take(pair_slots.at[pl.ds(0, CHIPS - 1)], sent)
    take(pair_in, sent)


def write_kernel(g, u, a, b, g_out, u_out, a_out, b_out, sem):
    parts = 16
    rows = g.shape[0] // parts
    copies = []
    for k in range(parts):
        where = pl.ds(k * rows, rows)
        copies.append(pltpu.make_async_copy(g.at[where], g_out.at[where], sem))
        copies.append(pltpu.make_async_copy(u.at[where], u_out.at[where], sem))
    copies.append(pltpu.make_async_copy(a, a_out, sem))
    copies.append(pltpu.make_async_copy(b, b_out, sem))
    for copy in copies:
        copy.start()
    for copy in copies:
        copy.wait()


def shards(weight_gate, moment_gate, square_gate, weight_up, moment_up, square_up, norm_gain):
    rows, width = weight_gate.shape
    total_rows = rows * lax.axis_size("rows")
    any_spec = pl.BlockSpec(memory_space=pl.ANY)
    hbm_spec = pl.BlockSpec(memory_space=pltpu.HBM)
    vmem_spec = pl.BlockSpec(memory_space=pltpu.VMEM)
    dma = pltpu.SemaphoreType.DMA
    g, u, a, b = pl.pallas_call(
        gather_kernel,
        name="gather",
        out_shape=(
            pltpu.VMEM((total_rows, width), BF16),
            pltpu.VMEM((total_rows, width), BF16),
            pltpu.VMEM((1, width), F32),
            pltpu.VMEM((1, width), F32),
        ),
        in_specs=[hbm_spec] * 7,
        out_specs=(vmem_spec,) * 4,
        scratch_shapes=[
            pltpu.VMEM((2, 3, rows, width), F32),
            pltpu.VMEM((2, rows, width), F32),
            pltpu.VMEM((1, rows), F32),
            pltpu.VMEM((rows, rows), F32),
            pltpu.VMEM((2, 1, width), F32),
            pltpu.VMEM((2 * CHIPS, 1, width // GROUPS), F32),
            pltpu.VMEM((GROUPS - 1, 1, width // GROUPS), F32),
            pltpu.VMEM((CHIPS, GROUPS - 1, 1, width // GROUPS), F32),
            pltpu.VMEM((2, RAW, width // GROUPS), F32),
            dma((AHEAD + 1,)), dma, dma, dma, dma((2,)), dma((2,)), dma((2,)), dma((2,)),
            dma((2, CHIPS // 2 - 1, 2)), dma((2, PIECES // 2)), dma,
        ],
        compiler_params=pltpu.CompilerParams(
            collective_id=0, has_side_effects=True, vmem_limit_bytes=47 * 2**20
        ),
    )(weight_gate, moment_gate, square_gate, weight_up, moment_up, square_up, norm_gain.reshape(1, rows))
    g, u, a, b = pl.pallas_call(
        write_kernel,
        name="write",
        out_shape=(
            jax.ShapeDtypeStruct((total_rows, width), BF16),
            jax.ShapeDtypeStruct((total_rows, width), BF16),
            jax.ShapeDtypeStruct((1, width), F32),
            jax.ShapeDtypeStruct((1, width), F32),
        ),
        in_specs=[vmem_spec] * 4,
        out_specs=(any_spec,) * 4,
        scratch_shapes=[dma],
        compiler_params=pltpu.CompilerParams(vmem_limit_bytes=2 * 2**20),
    )(g, u, a, b)
    return g, u, a.reshape(width), b.reshape(width)


def solution(mesh):
    return jax.shard_map(
        shards,
        mesh=mesh,
        in_specs=(
            P(("trial", "rows"), "cols"),
            P(("trial", "rows"), "cols"),
            P(("trial", "rows"), "cols"),
            P(("trial", "rows"), "cols"),
            P(("trial", "rows"), "cols"),
            P(("trial", "rows"), "cols"),
            P(("trial", "rows")),
        ),
        out_specs=(
            P("trial", "cols"),
            P("trial", "cols"),
            P(("trial", "cols")),
            P(("trial", "cols")),
        ),
        check_vma=False,
    )
```

```python
import functools

import jax
import jax.numpy as jnp
from jax import lax
from jax.experimental import pallas as pl
from jax.experimental.pallas import tpu as pltpu
from jax.sharding import PartitionSpec as P

D_MODEL = 2048
learn_rate = 0.02
decay_rate = 0.05
tiny_value = 1e-08

MESH = pl.DeviceIdType.MESH
F32, BF16 = jnp.float32, jnp.bfloat16

CHIPS = 8
GROUPS = 4
PIECES = 8
LAST = 5
CHUNK = 512
AHEAD = 3
RAW = 80
SLICES = ((0, 1, 2), (), (), (3, 4))
SLICE = 16


def gather_kernel(
    wg, mg, sg, wu, mu, su, gain_hbm,
    out_g, out_u, scale_g, scale_u,
    held, plain, gain, gain_t, part, slots, pair_in, pair_slots, raw_in,
    load_sem, gain_sem, sent, pair_r, slot_r, scale_r, raw_r, rest_r, ring_r, last_r, side_r,
):
    rows, width = wg.shape
    wide = width * 2 // GROUPS
    half = wide // 2
    chunks = width // CHUNK
    me = lax.axis_index("rows")
    chip, core = me // 2, me % 2
    partner = chip * 2 + (1 - core)
    outs, scales = (out_g, out_u), (scale_g, scale_u)
    sources = ((wg, mg, sg), (wu, mu, su))

    def at(c):
        return lax.rem(c + CHIPS, CHIPS)

    def device(r):
        return dict(device_id={"rows": r}, device_id_type=MESH)

    def take(ref, sem):
        pltpu.make_async_copy(ref, ref, sem).wait()

    def load(n):
        q, k = n // chunks, n % chunks
        cols = pl.ds(k * CHUNK, CHUNK)
        for i in range(3):
            pltpu.make_async_copy(
                sources[q][i].at[:, cols], held.at[q, i, :, cols], load_sem.at[n % (AHEAD + 1)]
            ).start()

    barrier = pltpu.get_barrier_semaphore()
    for d in (4, 3, 5, 2, 6, 1, 7):
        for h in range(2):
            pl.semaphore_signal(barrier, inc=1, **device(at(chip + d) * 2 + h))
    pl.semaphore_signal(barrier, inc=1, **device(partner))

    gain_copy = pltpu.make_async_copy(gain_hbm, gain, gain_sem)
    gain_copy.start()
    for n in range(AHEAD):
        load(n)

    gain_copy.wait()
    gain_t[...] = jnp.broadcast_to(gain[...], (rows, rows)).T

    def update(n):
        q, k = n // chunks, n % chunks
        if n + AHEAD < 2 * chunks:
            load(n + AHEAD)
        block = held.at[q, :, :, pl.ds(k * CHUNK, CHUNK)]
        pltpu.make_async_copy(block, block, load_sem.at[n % (AHEAD + 1)]).wait()

        @pl.loop(k * CHUNK // 128, (k + 1) * CHUNK // 128)
        def _(j):
            cols = pl.ds(pl.multiple_of(j * 128, 128), 128)
            w = held[q, 0, :, cols]
            m = held[q, 1, :, cols]
            s = held[q, 2, :, cols]
            whole = w - learn_rate * (m / (jnp.sqrt(s) + tiny_value) + decay_rate * w)
            gained = whole * gain_t[...]
            plain[q, :, cols] = gained
            part[q, :, cols] = jnp.sum(jnp.abs(gained), axis=0, keepdims=True)

    def start_of(g, h):
        return (g % (GROUPS // 2)) * wide + (core + h) % 2 * half

    def cols_of(g, h):
        return pl.ds(pl.multiple_of(start_of(g, h), half), half)

    far_first = (4, 3, 5, 2, 6, 1, 7)

    def part_of(g, where):
        return part.at[g // (GROUPS // 2), :, where]

    def first_copy(where, target):
        return pltpu.make_async_remote_copy(
            src_ref=part_of(0, where), dst_ref=slots.at[me],
            send_sem=sent, recv_sem=slot_r.at[0], **device(target),
        )

    def send_first():
        for d in far_first:
            for h in range(2):
                first_copy(pl.ds(h * half, half), at(chip + d) * 2 + h).start()
        first_copy(cols_of(0, 1), partner).start()
        slots[me] = part[0, :, cols_of(0, 0)]

    rest = range(1, GROUPS)

    def pair_copy(g):
        return pltpu.make_async_remote_copy(
            src_ref=part_of(g, cols_of(g, 1)), dst_ref=pair_in.at[g - 1],
            send_sem=sent, recv_sem=pair_r, **device(partner),
        )

    def send_rest():
        take(pair_in, pair_r)
        for g in rest:
            pair_slots[chip, g - 1] = part_of(g, cols_of(g, 0))[...] + pair_in[g - 1]
        ref = pair_slots.at[chip]
        for d in far_first:
            pltpu.make_async_remote_copy(
                src_ref=ref, dst_ref=ref, send_sem=sent, recv_sem=slot_r.at[1],
                **device(at(chip + d) * 2 + core),
            ).start()

    def scale_copy(g):
        ref = scales[g // (GROUPS // 2)].at[:, cols_of(g, 0)]
        return pltpu.make_async_remote_copy(
            src_ref=ref, dst_ref=ref, send_sem=sent, recv_sem=scale_r.at[min(g, 1)],
            **device(partner),
        )

    def total_first():
        take(slots.at[pl.ds(0, 2 * CHIPS - 1)], slot_r.at[0])
        acc = slots[0]
        for r in range(1, 2 * CHIPS):
            acc = acc + slots[r]
        scale_g[:, cols_of(0, 0)] = acc / D_MODEL
        scale_copy(0).start()

    def total_rest():
        take(pair_slots.at[pl.ds(0, CHIPS - 1)], slot_r.at[1])
        for g in rest:
            acc = pair_slots[0, g - 1]
            for r in range(1, CHIPS):
                acc = acc + pair_slots[r, g - 1]
            scales[g // (GROUPS // 2)][:, cols_of(g, 0)] = acc / D_MODEL
            scale_copy(g).start()

    def rows_of(offset, first=0, count=rows):
        start = (at(chip + offset) * 2 + core) * rows + first
        return pl.ds(pl.multiple_of(start, SLICE), count)

    def place(offset, g):
        cols = pl.ds((g % (GROUPS // 2)) * wide, wide)
        return outs[g * 2 // GROUPS].at[rows_of(offset), cols]

    def neighbour(way):
        return device(at(chip + 1 - 2 * way) * 2 + core)

    def onward(ref, way, recv_sem):
        return pltpu.make_async_remote_copy(
            src_ref=ref, dst_ref=ref, send_sem=sent, recv_sem=recv_sem, **neighbour(way)
        )

    def raw_copy(i, way):
        some = pl.ds(i * SLICE, SLICE)
        return pltpu.make_async_remote_copy(
            src_ref=plain.at[0, some, cols_of(0, 0)], dst_ref=raw_in.at[way, some],
            send_sem=sent, recv_sem=raw_r.at[way], **neighbour(way),
        )

    def send_raw(turn):
        for i in SLICES[turn]:
            for way in range(2):
                raw_copy(i, way).start()

    def side_copy(ref):
        return pltpu.make_async_remote_copy(
            src_ref=ref, dst_ref=ref, send_sem=sent, recv_sem=side_r, **device(partner)
        )

    def narrow(p):
        g, h = p // 2, p % 2
        q = g // (GROUPS // 2)
        first = start_of(g, h)
        start = pl.multiple_of(me * rows, rows)

        @pl.loop(0, half // 128)
        def _(j):
            cols = pl.ds(pl.multiple_of(first + j * 128, 128), 128)
            inverse = 1.0 / scales[q][:, cols]
            outs[q][pl.ds(start, rows), cols] = (plain[q, :, cols] * inverse).astype(BF16)

    def unit_of(g, way):
        return orders[way].index(g) // 2

    def send_way(p, way):
        g = p // 2
        if p == 0:
            ref = outs[0].at[rows_of(0, RAW, rows - RAW), cols_of(0, 0)]
            onward(ref, way, rest_r.at[way]).start()
        else:
            ref = outs[g * 2 // GROUPS].at[rows_of(0), cols_of(g, p % 2)]
            onward(ref, way, ring_r.at[way, 0, unit_of(g, way)]).start()

    def send_own(p):
        g = p // 2
        narrow(p)
        send_way(p, 0)
        if g != late:
            send_way(p, 1)
        side_copy(outs[g * 2 // GROUPS].at[rows_of(0), cols_of(g, p % 2)]).start()

    late = 1
    orders = ((0, 1, 2, 3), (0, 2, 3, 1))
    each = 2 * chunks // GROUPS
    for n in range(each):
        update(n)
    pl.semaphore_wait(barrier, 2 * CHIPS - 1)
    send_first()
    send_raw(0)
    for g in rest:
        for n in range(g * each, (g + 1) * each):
            update(n)
        pair_copy(g).start()
        if g < GROUPS - 1:
            send_raw(g)
    send_rest()
    send_raw(GROUPS - 1)
    total_first()
    send_own(0)
    take(scale_g.at[:, cols_of(0, 0)], scale_r.at[0])
    send_own(1)
    total_rest()
    send_own(2)
    take(scale_g.at[:, pl.ds(0, half * (GROUPS - 1))], scale_r.at[1])
    for p in range(3, PIECES):
        send_own(p)
    for h in range(2):
        send_way(2 * late + h, 1)
    def scale_raw(way):
        take(raw_in.at[way, pl.ds(0, RAW)], raw_r.at[way])
        take(out_g.at[pl.ds(0, rows - RAW), pl.ds(0, half)], rest_r.at[way])

        @pl.loop(0, half // 128)
        def _(j):
            here = pl.ds(pl.multiple_of(j * 128, 128), 128)
            cols = pl.ds(pl.multiple_of(start_of(0, 0) + j * 128, 128), 128)
            inverse = 1.0 / scale_g[:, cols]
            out_g[rows_of(2 * way - 1, 0, RAW), cols] = (
                raw_in[way, pl.ds(0, RAW), here] * inverse
            ).astype(BF16)

    steps = CHIPS // 2
    farthest = ((0, 1), (2, 3))

    def last_pieces(offset, way, g):
        if g == farthest[way][0]:
            return [(0, place(offset, g))]
        cols = [pl.ds((g % (GROUPS // 2)) * wide + i * half, half) for i in range(2)]
        return [
            (1 + 2 * i + j, outs[g * 2 // GROUPS].at[rows_of(offset, j * rows // 2, rows // 2), cols[i]])
            for i in range(2)
            for j in range(2)
        ]

    for step in range(steps - 1):
        for unit in range(2):
            for way in range(2):
                offset = (2 * way - 1) * (step + 1)
                groups = orders[way][2 * unit : 2 * unit + 2]
                if step == 0 and unit == 0:
                    scale_raw(way)
                    take(out_g.at[pl.ds(0, rows), pl.ds(0, width - half)], ring_r.at[way, step, unit])
                else:
                    take(out_g.at[pl.ds(0, rows)], ring_r.at[way, step, unit])
                for g in groups:
                    if step + 1 < steps - 1:
                        onward(place(offset, g), way, ring_r.at[way, step + 1, unit]).start()
                    elif g in farthest[way]:
                        for k, ref in last_pieces(offset, way, g):
                            onward(ref, way, last_r.at[way, k]).start()
                    side_copy(place(offset, g)).start()
    for turn in range(LAST):
        for way in range(2):
            k, ref = [piece for g in farthest[way] for piece in last_pieces(steps, way, g)][turn]
            take(ref, last_r.at[way, k])
            side_copy(ref).start()
    take(out_g, side_r)
    take(out_g, sent)
    for way in range(2):
        take(out_g.at[pl.ds(0, rows * (CHIPS - 1) - rows * half // width)], sent)
    take(raw_in, sent)
    take(out_g.at[pl.ds(0, 2 * (rows - RAW)), pl.ds(0, half)], sent)
    take(scale_g.at[:, pl.ds(0, half * GROUPS)], sent)
    take(slots.at[pl.ds(0, 2 * CHIPS - 1)], sent)
    take(pair_slots.at[pl.ds(0, CHIPS - 1)], sent)
    take(pair_in, sent)


def write_kernel(g, u, a, b, g_out, u_out, a_out, b_out, sem):
    parts = 32
    rows = g.shape[0] // parts
    copies = []
    for k in range(parts):
        where = pl.ds(k * rows, rows)
        copies.append(pltpu.make_async_copy(g.at[where], g_out.at[where], sem))
        copies.append(pltpu.make_async_copy(u.at[where], u_out.at[where], sem))
    copies.append(pltpu.make_async_copy(a, a_out, sem))
    copies.append(pltpu.make_async_copy(b, b_out, sem))
    for copy in copies:
        copy.start()
    for copy in copies:
        copy.wait()


def shards(weight_gate, moment_gate, square_gate, weight_up, moment_up, square_up, norm_gain):
    rows, width = weight_gate.shape
    total_rows = rows * lax.axis_size("rows")
    any_spec = pl.BlockSpec(memory_space=pl.ANY)
    hbm_spec = pl.BlockSpec(memory_space=pltpu.HBM)
    vmem_spec = pl.BlockSpec(memory_space=pltpu.VMEM)
    dma = pltpu.SemaphoreType.DMA
    g, u, a, b = pl.pallas_call(
        gather_kernel,
        name="gather",
        out_shape=(
            pltpu.VMEM((total_rows, width), BF16),
            pltpu.VMEM((total_rows, width), BF16),
            pltpu.VMEM((1, width), F32),
            pltpu.VMEM((1, width), F32),
        ),
        in_specs=[hbm_spec] * 7,
        out_specs=(vmem_spec,) * 4,
        scratch_shapes=[
            pltpu.VMEM((2, 3, rows, width), F32),
            pltpu.VMEM((2, rows, width), F32),
            pltpu.VMEM((1, rows), F32),
            pltpu.VMEM((rows, rows), F32),
            pltpu.VMEM((2, 1, width), F32),
            pltpu.VMEM((2 * CHIPS, 1, width // GROUPS), F32),
            pltpu.VMEM((GROUPS - 1, 1, width // GROUPS), F32),
            pltpu.VMEM((CHIPS, GROUPS - 1, 1, width // GROUPS), F32),
            pltpu.VMEM((2, RAW, width // GROUPS), F32),
            dma((AHEAD + 1,)), dma, dma, dma, dma((2,)), dma((2,)), dma((2,)), dma((2,)),
            dma((2, CHIPS // 2 - 1, 2)), dma((2, LAST)), dma,
        ],
        compiler_params=pltpu.CompilerParams(
            collective_id=0, has_side_effects=True, vmem_limit_bytes=47 * 2**20
        ),
    )(weight_gate, moment_gate, square_gate, weight_up, moment_up, square_up, norm_gain.reshape(1, rows))
    g, u, a, b = pl.pallas_call(
        write_kernel,
        name="write",
        out_shape=(
            jax.ShapeDtypeStruct((total_rows, width), BF16),
            jax.ShapeDtypeStruct((total_rows, width), BF16),
            jax.ShapeDtypeStruct((1, width), F32),
            jax.ShapeDtypeStruct((1, width), F32),
        ),
        in_specs=[vmem_spec] * 4,
        out_specs=(any_spec,) * 4,
        scratch_shapes=[dma],
        compiler_params=pltpu.CompilerParams(vmem_limit_bytes=2 * 2**20),
    )(g, u, a, b)
    return g, u, a.reshape(width), b.reshape(width)


def solution(mesh):
    return jax.shard_map(
        shards,
        mesh=mesh,
        in_specs=(
            P(("trial", "rows"), "cols"),
            P(("trial", "rows"), "cols"),
            P(("trial", "rows"), "cols"),
            P(("trial", "rows"), "cols"),
            P(("trial", "rows"), "cols"),
            P(("trial", "rows"), "cols"),
            P(("trial", "rows")),
        ),
        out_specs=(
            P("trial", "cols"),
            P("trial", "cols"),
            P(("trial", "cols")),
            P(("trial", "cols")),
        ),
        check_vma=False,
    )
```
